32 devices in a mesh: gx: 4 (over z), gy: 4 (over y, x), gz: 2 (over core).
Axes of the slice: x: 2, y: 2, z: 4, core: 2. Of those that a mesh axis runs over, the one named last changes fastest.
Arguments:
- patch_logits: bfloat16 [4, 4, 2, 24, 20736], P('gx', 'gy', 'gz'), may hold values from -12 to 312
- patch_start: int32 [4, 4, 2, 3], replicated, may hold values from 0 to 112, as said below
- patch_owner: int32 [4, 4, 2], replicated, may hold values from 0 to 15, as said below
Outputs:
- probs: float32 [32, 128, 3, 256], P('gx', 'gy', None, 'gz')
The draws below stay inside these ranges and needn't reach their ends.
Inputs may be any that keep to these rules, and one draw needn't show every extreme that they name: `patch_start`: entry [i, j, k, d] is the first cell along dimension d of the patch at lattice position (i, j, k): i * 8 - 8 along x (32 and 128 in place of 8 along y and z), moved by at most 4 cells, then moved inward so that the patch lies inside the volume. `patch_owner`: for every k the entries [:, :, k] are the numbers 0 to 15, each once.
All inputs are finite; a program needn't handle non-finite values.
Results may differ from the reference program's by a relative error of at most 0.0003.
Values may be sent and summed in bfloat16 or wider, within the bound.
A program may use at most 128 MiB of HBM per device.

```python
import jax
import jax.numpy as jnp
from jax import lax

CLASSES = 3
BX = 8
BY = 32
BZ = 128
HALO = 8
JITTER = 4
KX = 4
KY = 4
KZ = 2
NX = 32
NY = 128
NZ = 256
PX = 24
PY = 48
PZ = 144


def draw_patch_logits(key, part):
    full_shape = (KX, KY, KZ, PX, PY, CLASSES, PZ)
    normal_key, spike_key = jax.random.split(jax.random.fold_in(key, 11))
    values = jnp.clip(2.0 * jax.random.normal(normal_key, full_shape, jnp.float32), -12.0, 12.0)
    return values.reshape(KX, KY, KZ, PX, PY * CLASSES * PZ).astype(jnp.bfloat16)


def draw_patch_start(key, part):
    subkeys = jax.random.split(jax.random.fold_in(key, 23), 3)
    counts = (KX, KY, KZ)
    blocks = (BX, BY, BZ)
    extents = (PX, PY, PZ)
    columns = []
    for dimension in range(3):
        lattice = lax.broadcasted_iota(jnp.int32, (KX, KY, KZ), dimension)
        jitter_cells = jax.random.randint(subkeys[dimension], (KX, KY, KZ), -JITTER, JITTER + 1)
        first_cell = lattice * blocks[dimension] - HALO + jitter_cells
        first_cell = jnp.clip(first_cell, 0, counts[dimension] * blocks[dimension] - extents[dimension])
        columns.append(first_cell)
    return jnp.stack(columns, axis=-1).astype(jnp.int32)


def draw_patch_owner(key, part):
    subkeys = jax.random.split(jax.random.fold_in(key, 37), KZ)

    def shuffled(subkey):
        return jax.random.permutation(subkey, KX * KY)
    orders = jax.vmap(shuffled)(subkeys)
    return jnp.transpose(orders).reshape(KX, KY, KZ).astype(jnp.int32)


def setup_inputs(seed: int = 0) -> dict:
    streams_of = jax.random.split(jax.random.key(seed), 4)
    return {
        "patch_logits": draw_patch_logits(jax.random.fold_in(streams_of[3], 71), 0),
        "patch_start": draw_patch_start(jax.random.fold_in(streams_of[3], 71), 0),
        "patch_owner": draw_patch_owner(jax.random.fold_in(streams_of[3], 71), 0),
    }


def profile(length):
    offsets = jnp.arange(length).astype(jnp.float32)
    centre = (length - 1) / 2.0
    spread = length / 4.0
    return jnp.exp(-((offsets - centre) ** 2) / (2.0 * spread * spread))


def reference(patch_logits, patch_start, patch_owner):
    weight = profile(PX)[:, None, None, None] * profile(PY)[None, :, None, None]
    weight = weight * profile(PZ)[None, None, None, :]
    weight_full = jnp.broadcast_to(weight, (PX, PY, 1, PZ))
    totals = jnp.zeros((NX, NY, CLASSES + 1, NZ), jnp.float32)

    def add_patch(flat_index, totals):
        along_x = flat_index // (KY * KZ)
        along_y = (flat_index // KZ) % KY
        along_z = flat_index % KZ
        patch_code = patch_owner[along_x, along_y, along_z]
        home_x = patch_code // KY
        home_y = patch_code % KY
        corner = patch_start[home_x, home_y, along_z].astype(jnp.int32)
        logits = patch_logits[along_x, along_y, along_z].astype(jnp.float32).reshape(PX, PY, CLASSES, PZ)
        contribution = jnp.concatenate([logits * weight, weight_full], axis=2)
        anchor = (corner[0], corner[1], jnp.int32(0), corner[2])
        current = lax.dynamic_slice(totals, anchor, (PX, PY, CLASSES + 1, PZ))
        return lax.dynamic_update_slice(totals, current + contribution, anchor)

    totals = lax.fori_loop(0, KX * KY * KZ, add_patch, totals)
    scores = totals[:, :, :CLASSES] / totals[:, :, CLASSES:]
    return jax.nn.softmax(scores, axis=2)
```

```python
import functools

import jax
import jax.numpy as jnp
from jax import lax
from jax.experimental import pallas as pl
from jax.experimental.pallas import tpu as pltpu
from jax.sharding import PartitionSpec as P

CLASSES = 3
BX = 8
BY = 32
BZ = 128
HALO = 8
PX = 24
PY = 48
PZ = 144
RIM = PZ - BZ
ROWS = CLASSES + 1
GROUP = 8


def profile(offsets, length):
    inside = (offsets >= 0) & (offsets < length)
    centre = (length - 1) / 2.0
    spread = length / 4.0
    values = jnp.exp(-((offsets.astype(jnp.float32) - centre) ** 2) / (2.0 * spread * spread))
    return jnp.where(inside, values, 0.0)


def pack_kernel(lanes_x, place_ref, logits_ref, out_ref):
    start_x = place_ref[0]
    shift_z = place_ref[1]
    rows = lanes_x * BX
    r = lax.broadcasted_iota(jnp.int32, (rows, PX), 0)
    p = lax.broadcasted_iota(jnp.int32, (rows, PX), 1)
    pick = jnp.where(r - start_x == p, 1.0, 0.0).astype(jnp.bfloat16)
    width = GROUP * CLASSES * PZ
    fill = jnp.zeros((rows, 2 * BZ - PZ), jnp.float32)

    def step(g, carry):
        lanes = pl.ds(pl.multiple_of(g * width, 128), width)
        cells = jnp.dot(pick, logits_ref[:, lanes], preferred_element_type=jnp.float32)
        for y in range(GROUP):
            rims = None
            for c in range(CLASSES):
                at = (y * CLASSES + c) * PZ
                line = jnp.concatenate([cells[:, at : at + PZ], fill], axis=1)
                line = pltpu.roll(line, 2 * BZ - shift_z, 1)
                main = line[:, :BZ].astype(jnp.bfloat16)
                rim = pltpu.roll(line[:, BZ:], RIM + 2 * RIM * c, 1)
                rims = rim if rims is None else rims + rim
                for t in range(lanes_x):
                    out_ref[t, g * GROUP + y, c] = main[t * BX : (t + 1) * BX]
            rims = rims.astype(jnp.bfloat16)
            for t in range(lanes_x):
                out_ref[t, g * GROUP + y, CLASSES] = rims[t * BX : (t + 1) * BX]
        return carry

    lax.fori_loop(0, PY // GROUP, step, 0)


def blend_kernel(lanes_x, lanes_y, start_ref, along_y_ref, plane_ref, cells_ref, out_ref):
    def step(row, carry):
        sums = [None] * ROWS
        for p in range(lanes_x):
            q = jnp.clip(row - start_ref[p], 0, PY - 1)
            w = along_y_ref[p, row]
            main = plane_ref[p, 0] * w
            rim = plane_ref[p, 1] * w
            for c in range(ROWS):
                term = cells_ref[p, q, c].astype(jnp.float32) * (main if c < CLASSES else rim)
                sums[c] = term if sums[c] is None else sums[c] + term
        for c in range(ROWS):
            out_ref[row // BY, row % BY, c] = sums[c]
        return carry

    lax.fori_loop(0, lanes_y * BY, step, 0)


def finish_kernel(parts_ref, below_ref, above_ref, weight_ref, out_ref):
    lane = lax.broadcasted_iota(jnp.int32, (BX, BZ), 1)

    def step(y, carry):
        scale = 1.0 / weight_ref[y]
        below = below_ref[y]
        above = above_ref[y]
        scores = []
        for c in range(CLASSES):
            low = pltpu.roll(below, BZ - (2 * RIM * c + RIM), 1)
            high = pltpu.roll(above, BZ - RIM - 2 * RIM * c, 1)
            total = parts_ref[y, c] + jnp.where(lane < RIM, low, 0.0)
            total = total + jnp.where(lane >= BZ - RIM, high, 0.0)
            scores.append(total * scale)
        top = functools.reduce(jnp.maximum, scores)
        powers = [jnp.exp(s - top) for s in scores]
        norm = 1.0 / functools.reduce(jnp.add, powers)
        for c in range(CLASSES):
            out_ref[y, c] = powers[c] * norm
        return carry

    lax.fori_loop(0, BY, step, 0)


VMEM = pl.BlockSpec(memory_space=pltpu.VMEM)
SMEM = pl.BlockSpec(memory_space=pltpu.SMEM)


def per_device(patch_logits, patch_start, patch_owner):
    lanes_x = lax.axis_size("gx")
    lanes_y = lax.axis_size("gy")
    lanes_z = lax.axis_size("gz")
    place_x = lax.axis_index("gx")
    place_y = lax.axis_index("gy")
    place_z = lax.axis_index("gz")
    cells_y = lanes_y * BY
    codes = patch_owner[:, place_y, place_z]
    corners = patch_start[codes // lanes_y, codes % lanes_y, place_z]
    corner = corners[place_x]
    place = jnp.stack([corner[0], place_z * BZ - corner[2]])
    packed = pl.pallas_call(
        functools.partial(pack_kernel, lanes_x),
        out_shape=jax.ShapeDtypeStruct((lanes_x, PY, ROWS, BX, BZ), jnp.bfloat16),
        in_specs=[SMEM, VMEM],
        out_specs=VMEM,
    )(place, patch_logits[0, 0, 0])
    arrived = lax.all_to_all(packed, "gx", split_axis=0, concat_axis=0, tiled=True)

    along_x = profile(place_x * BX + jnp.arange(BX)[None, :] - corners[:, 0:1], PX)
    along_y = profile(jnp.arange(cells_y)[None, :] - corners[:, 1:2], PY)
    shift = place_z * BZ - corners[:, 2:3]
    main_z = profile(jnp.arange(BZ)[None, :] + shift, PZ)
    j = jnp.arange(RIM)[None, :]
    rim_z = jnp.concatenate([profile(j + shift - RIM, PZ), profile(BZ + j + shift, PZ)], axis=1)
    rim_z = jnp.pad(jnp.tile(rim_z, (1, CLASSES)), ((0, 0), (0, BZ - 2 * RIM * CLASSES)))
    plane = along_x[:, None, :, None] * jnp.stack([main_z, rim_z], axis=1)[:, :, None, :]
    parts = pl.pallas_call(
        functools.partial(blend_kernel, lanes_x, lanes_y),
        out_shape=jax.ShapeDtypeStruct((lanes_y, BY, ROWS, BX, BZ), jnp.float32),
        in_specs=[SMEM, SMEM, VMEM, VMEM],
        out_specs=VMEM,
    )(corners[:, 1], along_y, plane, arrived)
    parts = lax.all_to_all(parts, "gy", split_axis=0, concat_axis=0, tiled=True)
    parts = jnp.sum(parts, axis=0)

    layers = jnp.clip(place_z + jnp.arange(-1, 2), 0, lanes_z - 1)
    real = (place_z + jnp.arange(-1, 2) >= 0) & (place_z + jnp.arange(-1, 2) < lanes_z)
    near = jnp.take(patch_start, layers, axis=2)
    every_x = profile(place_x * BX + jnp.arange(BX) - near[..., 0:1], PX)
    every_y = profile(place_y * BY + jnp.arange(BY) - near[..., 1:2], PY)
    every_z = profile(place_z * BZ + jnp.arange(BZ) - near[..., 2:3], PZ)
    every_z = jnp.where(real[None, None, :, None], every_z, 0.0)
    every_y = every_y.reshape(-1, BY)
    every_xz = (every_x[..., :, None] * every_z[..., None, :]).reshape(-1, BX * BZ)
    weight = lax.dot_general(
        every_y, every_xz, (((0,), (0,)), ((), ())), precision=lax.Precision.HIGHEST
    ).reshape(BY, BX, BZ)

    rims = parts[:, CLASSES]
    up = [(i, i + 1) for i in range(lanes_z - 1)]
    down = [(j, i) for i, j in up]
    below = lax.ppermute(rims, "gz", up)
    above = lax.ppermute(rims, "gz", down)
    probs = pl.pallas_call(
        finish_kernel,
        out_shape=jax.ShapeDtypeStruct((BY, CLASSES, BX, BZ), jnp.float32),
        in_specs=[VMEM] * 4,
        out_specs=VMEM,
    )(parts, below, above, weight)
    return jnp.transpose(probs, (2, 0, 1, 3))


def solution(mesh):
    return jax.shard_map(
        per_device,
        mesh=mesh,
        in_specs=(P("gx", "gy", "gz", None, None), P(), P()),
        out_specs=P("gx", "gy", None, "gz"),
        check_vma=False,
    )
```

```python
import functools

import jax
import jax.numpy as jnp
from jax import lax
from jax.experimental import pallas as pl
from jax.experimental.pallas import tpu as pltpu
from jax.sharding import PartitionSpec as P

CLASSES = 3
BX = 8
BY = 32
BZ = 128
HALO = 8
PX = 24
PY = 48
PZ = 144
RIM = PZ - BZ
ROWS = CLASSES + 1
GROUP = 8
MESH = pl.DeviceIdType.MESH


def profile(offsets, length):
    inside = (offsets >= 0) & (offsets < length)
    centre = (length - 1) / 2.0
    spread = length / 4.0
    values = jnp.exp(-((offsets.astype(jnp.float32) - centre) ** 2) / (2.0 * spread * spread))
    return jnp.where(inside, values, 0.0)


def pack_kernel(lanes_x, place_ref, logits_ref, out_ref):
    start_x = place_ref[0]
    shift_z = place_ref[1]
    place_x = place_ref[2]
    rows = lanes_x * BX
    r = lax.broadcasted_iota(jnp.int32, (rows, PX), 0)
    p = lax.broadcasted_iota(jnp.int32, (rows, PX), 1)
    x = r + place_x * BX
    x = jnp.where(x >= rows, x - rows, x)
    pick = jnp.where(x - start_x == p, 1.0, 0.0).astype(jnp.bfloat16)
    width = GROUP * CLASSES * PZ
    fill = jnp.zeros((rows, 2 * BZ - PZ), jnp.float32)

    def step(g, carry):
        lanes = pl.ds(pl.multiple_of(g * width, 128), width)
        cells = jnp.dot(pick, logits_ref[:, lanes], preferred_element_type=jnp.float32)
        for y in range(GROUP):
            rims = None
            for c in range(CLASSES):
                at = (y * CLASSES + c) * PZ
                line = jnp.concatenate([cells[:, at : at + PZ], fill], axis=1)
                line = pltpu.roll(line, 2 * BZ - shift_z, 1)
                main = line[:, :BZ].astype(jnp.bfloat16)
                rim = pltpu.roll(line[:, BZ:], RIM + 2 * RIM * c, 1)
                rims = rim if rims is None else rims + rim
                for t in range(lanes_x):
                    out_ref[c, t, g * GROUP + y] = main[t * BX : (t + 1) * BX]
            rims = rims.astype(jnp.bfloat16)
            for t in range(lanes_x):
                out_ref[CLASSES, t, g * GROUP + y] = rims[t * BX : (t + 1) * BX]
        return carry

    lax.fori_loop(0, PY // GROUP, step, 0)


def blend_kernel(
    lanes_x, lanes_y, lanes_z,
    start_ref, along_y_ref, plane_ref, weight_ref, packed_ref, out_ref,
    land0, land1, land2, land3, parts, parts_land, rims, rims_land,
    cells_out, cells_in, parts_out, parts_in, rims_out, rims_in,
):
    place_x = lax.axis_index("gx")
    place_y = lax.axis_index("gy")
    place_z = lax.axis_index("gz")

    cells_land = (land0, land1, land2, land3)

    def ahead(place, d, size):
        return lax.rem(place + d, size)

    barrier = pltpu.get_barrier_semaphore()
    peers = [{"gx": ahead(place_x, d, lanes_x)} for d in range(1, lanes_x)]
    peers += [{"gy": ahead(place_y, d, lanes_y)} for d in range(1, lanes_y)]
    peers += [{"gz": ahead(place_z, d, lanes_z)} for d in (1, lanes_z - 1)]
    for peer in peers:
        pl.semaphore_signal(barrier, inc=1, device_id=peer, device_id_type=MESH)
    pl.semaphore_wait(barrier, len(peers))

    order = (CLASSES,) + tuple(range(CLASSES))
    far_x = sorted(range(1, lanes_x), key=lambda d: -min(d, lanes_x - d))
    far_y = sorted(range(1, lanes_y), key=lambda d: -min(d, lanes_y - d))
    cell_copies = {
        (c, d): pltpu.make_async_remote_copy(
            src_ref=packed_ref.at[c, d],
            dst_ref=cells_land[c].at[d],
            send_sem=cells_out.at[c, d],
            recv_sem=cells_in.at[c, d],
            device_id={"gx": ahead(place_x, d, lanes_x)},
            device_id_type=MESH,
        )
        for c in order
        for d in far_x
    }
    part_copies = {
        (c, d): pltpu.make_async_remote_copy(
            src_ref=parts.at[c, d],
            dst_ref=parts_land.at[c, d],
            send_sem=parts_out.at[c, d],
            recv_sem=parts_in.at[c, d],
            device_id={"gy": ahead(place_y, d, lanes_y)},
            device_id_type=MESH,
        )
        for c in order
        for d in far_y
    }
    rim_copies = [
        pltpu.make_async_remote_copy(
            src_ref=rims,
            dst_ref=rims_land.at[side],
            send_sem=rims_out.at[side],
            recv_sem=rims_in.at[side],
            device_id={"gz": ahead(place_z, d, lanes_z)},
            device_id_type=MESH,
        )
        for side, d in ((0, 1), (1, lanes_z - 1))
    ]
    for c in order:
        for d in far_x:
            cell_copies[c, d].start()

    def blend(c):
        kind = 0 if c < CLASSES else 1
        for d in far_y + [0]:
            base = ahead(place_y, d, lanes_y) * BY

            def step(y, carry):
                row = base + y
                total = None
                for p in range(lanes_x):
                    q = jnp.clip(row - start_ref[p], 0, PY - 1)
                    cells = packed_ref[c, 0, q] if p == 0 else cells_land[c][p, q]
                    term = cells.astype(jnp.float32) * (plane_ref[p, kind] * along_y_ref[p, row])
                    total = term if total is None else total + term
                parts[c, d, y] = total
                return carry

            lax.fori_loop(0, BY, step, 0, unroll=2)
            if d:
                part_copies[c, d].start()

    def gathered(c, y):
        total = parts[c, 0, y]
        for d in range(1, lanes_y):
            total = total + parts_land[c, d, y]
        return total

    for c in order:
        for d in far_x:
            cell_copies[c, d].wait_recv()
        blend(c)
        if c == 0:
            for d in far_y:
                part_copies[CLASSES, d].wait_recv()

            def add_rims(y, carry):
                rims[y] = gathered(CLASSES, y)
                return carry

            lax.fori_loop(0, BY, add_rims, 0)
            for copy in rim_copies:
                copy.start()

    for copy in rim_copies:
        copy.wait_recv()
    for c in range(CLASSES):
        for d in far_y:
            part_copies[c, d].wait_recv()

    lane = lax.broadcasted_iota(jnp.int32, (BX, BZ), 1)
    low_lanes = (lane < RIM) & (place_z > 0)
    high_lanes = (lane >= BZ - RIM) & (place_z < lanes_z - 1)

    def finish(y, carry):
        scale = 1.0 / weight_ref[y]
        below = rims_land[0, y]
        above = rims_land[1, y]
        scores = []
        for c in range(CLASSES):
            low = pltpu.roll(below, BZ - (2 * RIM * c + RIM), 1)
            high = pltpu.roll(above, BZ - RIM - 2 * RIM * c, 1)
            total = gathered(c, y) + jnp.where(low_lanes, low, 0.0)
            total = total + jnp.where(high_lanes, high, 0.0)
            scores.append(total * scale)
        top = functools.reduce(jnp.maximum, scores)
        powers = [jnp.exp(s - top) for s in scores]
        norm = 1.0 / functools.reduce(jnp.add, powers)
        for c in range(CLASSES):
            out_ref[y, c] = powers[c] * norm
        return carry

    lax.fori_loop(0, BY, finish, 0, unroll=2)
    for copy in list(cell_copies.values()) + list(part_copies.values()) + rim_copies:
        copy.wait_send()


VMEM = pl.BlockSpec(memory_space=pltpu.VMEM)
SMEM = pl.BlockSpec(memory_space=pltpu.SMEM)


def per_device(patch_logits, patch_start, patch_owner):
    lanes_x = lax.axis_size("gx")
    lanes_y = lax.axis_size("gy")
    lanes_z = lax.axis_size("gz")
    place_x = lax.axis_index("gx")
    place_y = lax.axis_index("gy")
    place_z = lax.axis_index("gz")
    cells_y = lanes_y * BY
    behind = lax.rem(place_x - jnp.arange(lanes_x) + lanes_x, lanes_x)
    codes = patch_owner[behind, place_y, place_z]
    corners = patch_start[codes // lanes_y, codes % lanes_y, place_z]
    place = jnp.stack([corners[0, 0], place_z * BZ - corners[0, 2], place_x])
    packed = pl.pallas_call(
        functools.partial(pack_kernel, lanes_x),
        out_shape=jax.ShapeDtypeStruct((ROWS, lanes_x, PY, BX, BZ), jnp.bfloat16),
        in_specs=[SMEM, VMEM],
        out_specs=VMEM,
    )(place, patch_logits[0, 0, 0])

    along_x = profile(place_x * BX + jnp.arange(BX)[None, :] - corners[:, 0:1], PX)
    along_y = profile(jnp.arange(cells_y)[None, :] - corners[:, 1:2], PY)
    shift = place_z * BZ - corners[:, 2:3]
    main_z = profile(jnp.arange(BZ)[None, :] + shift, PZ)
    j = jnp.arange(RIM)[None, :]
    rim_z = jnp.concatenate([profile(j + shift - RIM, PZ), profile(BZ + j + shift, PZ)], axis=1)
    rim_z = jnp.pad(jnp.tile(rim_z, (1, CLASSES)), ((0, 0), (0, BZ - 2 * RIM * CLASSES)))
    plane = along_x[:, None, :, None] * jnp.stack([main_z, rim_z], axis=1)[:, :, None, :]

    layers = jnp.clip(place_z + jnp.arange(-1, 2), 0, lanes_z - 1)
    real = (place_z + jnp.arange(-1, 2) >= 0) & (place_z + jnp.arange(-1, 2) < lanes_z)
    near = jnp.take(patch_start, layers, axis=2)
    every_x = profile(place_x * BX + jnp.arange(BX) - near[..., 0:1], PX)
    every_y = profile(place_y * BY + jnp.arange(BY) - near[..., 1:2], PY)
    every_z = profile(place_z * BZ + jnp.arange(BZ) - near[..., 2:3], PZ)
    every_z = jnp.where(real[None, None, :, None], every_z, 0.0)
    every_y = every_y.reshape(-1, BY)
    every_xz = (every_x[..., :, None] * every_z[..., None, :]).reshape(-1, BX * BZ)
    weight = lax.dot_general(
        every_y, every_xz, (((0,), (0,)), ((), ())), precision=lax.Precision.HIGHEST
    ).reshape(BY, BX, BZ)

    cells_shape = (lanes_x, PY, BX, BZ)
    parts_shape = (ROWS, lanes_y, BY, BX, BZ)
    probs = pl.pallas_call(
        functools.partial(blend_kernel, lanes_x, lanes_y, lanes_z),
        out_shape=jax.ShapeDtypeStruct((BY, CLASSES, BX, BZ), jnp.float32),
        in_specs=[SMEM, SMEM, VMEM, VMEM, VMEM],
        out_specs=VMEM,
        scratch_shapes=[
            *[pltpu.VMEM(cells_shape, jnp.bfloat16)] * ROWS,
            pltpu.VMEM(parts_shape, jnp.float32),
            pltpu.VMEM(parts_shape, jnp.float32),
            pltpu.VMEM((BY, BX, BZ), jnp.float32),
            pltpu.VMEM((2, BY, BX, BZ), jnp.float32),
            pltpu.SemaphoreType.DMA((ROWS, lanes_x)),
            pltpu.SemaphoreType.DMA((ROWS, lanes_x)),
            pltpu.SemaphoreType.DMA((ROWS, lanes_y)),
            pltpu.SemaphoreType.DMA((ROWS, lanes_y)),
            pltpu.SemaphoreType.DMA((2,)),
            pltpu.SemaphoreType.DMA((2,)),
        ],
        compiler_params=pltpu.CompilerParams(collective_id=0, has_side_effects=True),
    )(corners[:, 1], along_y, plane, weight, packed)
    return jnp.transpose(probs, (2, 0, 1, 3))


def solution(mesh):
    return jax.shard_map(
        per_device,
        mesh=mesh,
        in_specs=(P("gx", "gy", "gz", None, None), P(), P()),
        out_specs=P("gx", "gy", None, "gz"),
        check_vma=False,
    )
```

```python
import functools

import jax
import jax.numpy as jnp
from jax import lax
from jax.experimental import pallas as pl
from jax.experimental.pallas import tpu as pltpu
from jax.sharding import PartitionSpec as P

CLASSES = 3
BX = 8
BY = 32
BZ = 128
HALO = 8
PX = 24
PY = 48
PZ = 144
RIM = PZ - BZ
ROWS = CLASSES + 1
GROUP = 8
MESH = pl.DeviceIdType.MESH


def profile(offsets, length, keep=True):
    inside = (offsets >= 0) & (offsets < length) & keep
    centre = (length - 1) / 2.0
    spread = length / 4.0
    values = jnp.exp((offsets.astype(jnp.float32) - centre) ** 2 * (-0.5 / (spread * spread)))
    return jnp.where(inside, values, 0.0)


def corner_of(start_ref, code, lanes_y, layer):
    return [start_ref[code // lanes_y, code % lanes_y, layer, k] for k in range(3)]


def pack_kernel(lanes_x, lanes_y, start_ref, owner_ref, logits_ref, out_ref):
    place_x = lax.axis_index("gx")
    place_z = lax.axis_index("gz")
    code = owner_ref[place_x, lax.axis_index("gy"), place_z]
    start_x, _, start_z = corner_of(start_ref, code, lanes_y, place_z)
    shift_z = place_z * BZ - start_z
    rows = lanes_x * BX
    r = lax.broadcasted_iota(jnp.int32, (rows, PX), 0)
    p = lax.broadcasted_iota(jnp.int32, (rows, PX), 1)
    x = r + place_x * BX
    x = jnp.where(x >= rows, x - rows, x)
    pick = jnp.where(x - start_x == p, 1.0, 0.0).astype(jnp.bfloat16)
    width = GROUP * CLASSES * PZ
    fill = jnp.zeros((rows, 2 * BZ - PZ), jnp.float32)

    def step(g, carry):
        lanes = pl.ds(pl.multiple_of(g * width, 128), width)
        cells = jnp.dot(pick, logits_ref[:, lanes], preferred_element_type=jnp.float32)
        for y in range(GROUP):
            rims = None
            for c in range(CLASSES):
                at = (y * CLASSES + c) * PZ
                line = jnp.concatenate([cells[:, at : at + PZ], fill], axis=1)
                line = pltpu.roll(line, 2 * BZ - shift_z, 1)
                main = line[:, :BZ].astype(jnp.bfloat16)
                rim = pltpu.roll(line[:, BZ:], RIM + 2 * RIM * c, 1)
                rims = rim if rims is None else rims + rim
                for t in range(lanes_x):
                    out_ref[c, t, g * GROUP + y] = main[t * BX : (t + 1) * BX]
            rims = rims.astype(jnp.bfloat16)
            for t in range(lanes_x):
                out_ref[CLASSES, t, g * GROUP + y] = rims[t * BX : (t + 1) * BX]
        return carry

    lax.fori_loop(0, PY // GROUP, step, 0)


def blend_kernel(
    lanes_x, lanes_y, lanes_z,
    start_ref, owner_ref, packed_ref, out_ref, along_y_ref, plane_ref, weight_ref,
    land0, land1, land2, land3, parts, parts_land, rims, rims_land,
    cells_out, cells_in, parts_out, parts_in, rims_out, rims_in,
):
    place_x = lax.axis_index("gx")
    place_y = lax.axis_index("gy")
    place_z = lax.axis_index("gz")

    cells_land = (land0, land1, land2, land3)

    def ahead(place, d, size):
        return lax.rem(place + d, size)

    barrier = pltpu.get_barrier_semaphore()
    peers = [{"gx": ahead(place_x, d, lanes_x)} for d in range(1, lanes_x)]
    peers += [{"gy": ahead(place_y, d, lanes_y)} for d in range(1, lanes_y)]
    peers += [{"gz": ahead(place_z, d, lanes_z)} for d in (1, lanes_z - 1)]
    for peer in peers:
        pl.semaphore_signal(barrier, inc=1, device_id=peer, device_id_type=MESH)
    pl.semaphore_wait(barrier, len(peers))

    order = (CLASSES,) + tuple(range(CLASSES))
    far_x = sorted(range(1, lanes_x), key=lambda d: -min(d, lanes_x - d))
    far_y = sorted(range(1, lanes_y), key=lambda d: -min(d, lanes_y - d))
    cell_copies = {
        (c, d): pltpu.make_async_remote_copy(
            src_ref=packed_ref.at[c, d],
            dst_ref=cells_land[c].at[d],
            send_sem=cells_out.at[c, d],
            recv_sem=cells_in.at[c, d],
            device_id={"gx": ahead(place_x, d, lanes_x)},
            device_id_type=MESH,
        )
        for c in order
        for d in far_x
    }
    part_copies = {
        (c, d): pltpu.make_async_remote_copy(
            src_ref=parts.at[c, d],
            dst_ref=parts_land.at[c, d],
            send_sem=parts_out.at[c, d],
            recv_sem=parts_in.at[c, d],
            device_id={"gy": ahead(place_y, d, lanes_y)},
            device_id_type=MESH,
        )
        for c in order
        for d in far_y
    }
    rim_copies = [
        pltpu.make_async_remote_copy(
            src_ref=rims,
            dst_ref=rims_land.at[side],
            send_sem=rims_out.at[side],
            recv_sem=rims_in.at[side],
            device_id={"gz": ahead(place_z, d, lanes_z)},
            device_id_type=MESH,
        )
        for side, d in ((0, 1), (1, lanes_z - 1))
    ]
    for c in order:
        for d in far_x:
            cell_copies[c, d].start()

    sub = lax.broadcasted_iota(jnp.int32, (BX, BZ), 0)
    lane = lax.broadcasted_iota(jnp.int32, (BX, BZ), 1)
    cell_x = place_x * BX + sub
    cells_y = lanes_y * BY
    starts_y = []
    for p in range(lanes_x):
        source = lax.rem(place_x - p + lanes_x, lanes_x)
        code = owner_ref[source, place_y, place_z]
        start_x, start_y, start_z = corner_of(start_ref, code, lanes_y, place_z)
        starts_y.append(start_y)
        shift_z = place_z * BZ - start_z
        part = lane % (2 * RIM)
        rim_z = jnp.where(part < RIM, part - RIM, part - RIM + BZ) + shift_z
        along_x = profile(cell_x - start_x, PX)
        plane_ref[p, 0] = along_x * profile(lane + shift_z, PZ)
        plane_ref[p, 1] = along_x * profile(rim_z, PZ, lane < 2 * RIM * CLASSES)
        row = lax.broadcasted_iota(jnp.int32, (cells_y, BZ), 0)
        along_y_ref[p] = profile(row - start_y, PY)

    weight_ref[...] = jnp.zeros(weight_ref.shape, jnp.float32)
    cell_y = place_y * BY + lax.broadcasted_iota(jnp.int32, (BY, BZ), 0)

    def weigh(code, carry):
        for step in (-1, 0, 1):
            layer = jnp.clip(place_z + step, 0, lanes_z - 1)
            start_x, start_y, start_z = corner_of(start_ref, code, lanes_y, layer)
            along = profile(cell_y - start_y, PY)
            plane = profile(cell_x - start_x, PX) * profile(
                place_z * BZ + lane - start_z, PZ, layer == place_z + step
            )
            for y in range(BY):
                weight_ref[y] = weight_ref[y] + plane * along[y : y + 1]
        return carry

    lax.fori_loop(0, lanes_x * lanes_y, weigh, 0)

    def blend(c):
        kind = 0 if c < CLASSES else 1
        for d in far_y + [0]:
            base = ahead(place_y, d, lanes_y) * BY

            def step(y, carry):
                row = base + y
                total = None
                for p in range(lanes_x):
                    q = jnp.clip(row - starts_y[p], 0, PY - 1)
                    cells = packed_ref[c, 0, q] if p == 0 else cells_land[c][p, q]
                    term = cells.astype(jnp.float32) * (plane_ref[p, kind] * along_y_ref[p, pl.ds(row, 1)])
                    total = term if total is None else total + term
                parts[c, d, y] = total
                return carry

            lax.fori_loop(0, BY, step, 0, unroll=2)
            if d:
                part_copies[c, d].start()

    def gathered(c, y):
        total = parts[c, 0, y]
        for d in range(1, lanes_y):
            total = total + parts_land[c, d, y]
        return total

    for c in order:
        for d in far_x:
            cell_copies[c, d].wait_recv()
        blend(c)
        if c == 0:
            for d in far_y:
                part_copies[CLASSES, d].wait_recv()

            def add_rims(y, carry):
                rims[y] = gathered(CLASSES, y)
                return carry

            lax.fori_loop(0, BY, add_rims, 0)
            for copy in rim_copies:
                copy.start()

    for copy in rim_copies:
        copy.wait_recv()
    for c in range(CLASSES):
        for d in far_y:
            part_copies[c, d].wait_recv()

    low_lanes = (lane < RIM) & (place_z > 0)
    high_lanes = (lane >= BZ - RIM) & (place_z < lanes_z - 1)

    def finish(y, carry):
        scale = 1.0 / weight_ref[y]
        below = rims_land[0, y]
        above = rims_land[1, y]
        scores = []
        for c in range(CLASSES):
            low = pltpu.roll(below, BZ - (2 * RIM * c + RIM), 1)
            high = pltpu.roll(above, BZ - RIM - 2 * RIM * c, 1)
            total = gathered(c, y) + jnp.where(low_lanes, low, 0.0)
            total = total + jnp.where(high_lanes, high, 0.0)
            scores.append(total * scale)
        top = functools.reduce(jnp.maximum, scores)
        powers = [jnp.exp(s - top) for s in scores]
        norm = 1.0 / functools.reduce(jnp.add, powers)
        for c in range(CLASSES):
            out_ref[y, c] = powers[c] * norm
        return carry

    lax.fori_loop(0, BY, finish, 0, unroll=4)
    for copy in list(cell_copies.values()) + list(part_copies.values()) + rim_copies:
        copy.wait_send()


VMEM = pl.BlockSpec(memory_space=pltpu.VMEM)
SMEM = pl.BlockSpec(memory_space=pltpu.SMEM)


def per_device(patch_logits, patch_start, patch_owner):
    lanes_x = lax.axis_size("gx")
    lanes_y = lax.axis_size("gy")
    lanes_z = lax.axis_size("gz")
    packed = pl.pallas_call(
        functools.partial(pack_kernel, lanes_x, lanes_y),
        out_shape=jax.ShapeDtypeStruct((ROWS, lanes_x, PY, BX, BZ), jnp.bfloat16),
        in_specs=[SMEM, SMEM, VMEM],
        out_specs=VMEM,
    )(patch_start, patch_owner, patch_logits[0, 0, 0])

    cells_shape = (lanes_x, PY, BX, BZ)
    parts_shape = (ROWS, lanes_y, BY, BX, BZ)
    probs = pl.pallas_call(
        functools.partial(blend_kernel, lanes_x, lanes_y, lanes_z),
        out_shape=jax.ShapeDtypeStruct((BY, CLASSES, BX, BZ), jnp.float32),
        in_specs=[SMEM, SMEM, VMEM],
        out_specs=VMEM,
        scratch_shapes=[
            pltpu.VMEM((lanes_x, lanes_y * BY, BZ), jnp.float32),
            pltpu.VMEM((lanes_x, 2, BX, BZ), jnp.float32),
            pltpu.VMEM((BY, BX, BZ), jnp.float32),
            *[pltpu.VMEM(cells_shape, jnp.bfloat16)] * ROWS,
            pltpu.VMEM(parts_shape, jnp.float32),
            pltpu.VMEM(parts_shape, jnp.float32),
            pltpu.VMEM((BY, BX, BZ), jnp.float32),
            pltpu.VMEM((2, BY, BX, BZ), jnp.float32),
            pltpu.SemaphoreType.DMA((ROWS, lanes_x)),
            pltpu.SemaphoreType.DMA((ROWS, lanes_x)),
            pltpu.SemaphoreType.DMA((ROWS, lanes_y)),
            pltpu.SemaphoreType.DMA((ROWS, lanes_y)),
            pltpu.SemaphoreType.DMA((2,)),
            pltpu.SemaphoreType.DMA((2,)),
        ],
        compiler_params=pltpu.CompilerParams(collective_id=0, has_side_effects=True),
    )(patch_start, patch_owner, packed)
    return jnp.transpose(probs, (2, 0, 1, 3))


def solution(mesh):
    return jax.shard_map(
        per_device,
        mesh=mesh,
        in_specs=(P("gx", "gy", "gz", None, None), P(), P()),
        out_specs=P("gx", "gy", None, "gz"),
        check_vma=False,
    )
```

```python
import functools

import jax
import jax.numpy as jnp
from jax import lax
from jax.experimental import pallas as pl
from jax.experimental.pallas import tpu as pltpu
from jax.sharding import PartitionSpec as P

CLASSES = 3
BX = 8
BY = 32
BZ = 128
HALO = 8
PX = 24
PY = 48
PZ = 144
RIM = PZ - BZ
ROWS = CLASSES + 1
GROUP = 8
FOLD = PY // 2
MESH = pl.DeviceIdType.MESH


def profile(offsets, length, keep=True):
    inside = (offsets >= 0) & (offsets < length) & keep
    centre = (length - 1) / 2.0
    spread = length / 4.0
    values = jnp.exp((offsets.astype(jnp.float32) - centre) ** 2 * (-0.5 / (spread * spread)))
    return jnp.where(inside, values, 0.0)


def corner_of(start_ref, code, lanes_y, layer):
    return [start_ref[code // lanes_y, code % lanes_y, layer, k] for k in range(3)]


def pick_x(lanes_x, place_x, start_x, logits_ref, cells_ref):
    rows = lanes_x * BX
    r = lax.broadcasted_iota(jnp.int32, (rows, PX), 0)
    p = lax.broadcasted_iota(jnp.int32, (rows, PX), 1)
    x = r + place_x * BX
    x = jnp.where(x >= rows, x - rows, x)
    pick = jnp.where(x - start_x == p, 1.0, 0.0).astype(jnp.bfloat16)
    width = GROUP * CLASSES * PZ
    for g in range(PY // GROUP):
        lanes = slice(g * width, (g + 1) * width)
        cells = jnp.dot(pick, logits_ref[:, lanes], preferred_element_type=jnp.float32)
        cells_ref[:, lanes] = cells.astype(jnp.bfloat16)


def lines_of(cells_ref, lines, source, phase):
    k = lax.broadcasted_iota(jnp.int32, (2 * BZ, BZ), 0)
    move = jnp.where(k - phase * RIM == source, 1.0, 0.0).astype(jnp.bfloat16)
    starts = [line * PZ - phase * RIM for line in lines]
    cells = jnp.concatenate([cells_ref[:, at : at + 2 * BZ] for at in starts], axis=0)
    return jnp.dot(cells, move, preferred_element_type=jnp.float32)


def pack_rims(lanes_x, shift_z, cells_ref, sums_ref, out_ref):
    rows = lanes_x * BX
    phases = BZ // RIM
    n = lax.broadcasted_iota(jnp.int32, (2 * BZ, BZ), 1)
    source = n + shift_z + jnp.where(n + shift_z < RIM, BZ, -RIM)
    source = jnp.where(n < RIM, source, -4 * BZ)
    sums_ref[...] = jnp.zeros(sums_ref.shape, jnp.float32)
    for phase in range(phases):
        lines = [i for i in range(PY * CLASSES) if i % phases == phase]
        moved = lines_of(cells_ref, lines, source, phase)
        for i, line in enumerate(lines):
            y, c = divmod(line, CLASSES)
            rim = moved[i * rows : (i + 1) * rows]
            at = RIM * c + BZ // 2 * (y // FOLD)
            rim = pltpu.roll(rim, at, 1) if at else rim
            sums_ref[y % FOLD] = sums_ref[y % FOLD] + rim

    def convert(y, carry):
        sums = sums_ref[y].astype(jnp.bfloat16)
        for t in range(lanes_x):
            out_ref[t, y] = sums[t * BX : (t + 1) * BX]
        return carry

    lax.fori_loop(0, FOLD, convert, 0, unroll=2)


def pack_class(lanes_x, shift_z, c, cells_ref, out_ref):
    rows = lanes_x * BX
    phases = BZ // RIM
    source = lax.broadcasted_iota(jnp.int32, (2 * BZ, BZ), 1) + shift_z
    for phase in range(phases):
        ys = [y for y in range(PY) if (y * CLASSES + c) % phases == phase]
        moved = lines_of(cells_ref, [y * CLASSES + c for y in ys], source, phase)
        moved = moved.astype(jnp.bfloat16)
        for i, y in enumerate(ys):
            for t in range(lanes_x):
                at = i * rows + t * BX
                out_ref[t, y] = moved[at : at + BX]


def blend_kernel(
    lanes_x, lanes_y, lanes_z,
    start_ref, owner_ref, logits_ref, out_ref, along_y_ref, plane_ref, weight_ref,
    cells_ref, sums_ref, pack0, pack1, pack2, pack3, land0, land1, land2, land3, parts, parts_land, rims, rims_land,
    cells_out, cells_in, parts_out, parts_in, rims_out, rims_in,
):
    place_x = lax.axis_index("gx")
    place_y = lax.axis_index("gy")
    place_z = lax.axis_index("gz")

    packed = (pack0, pack1, pack2, pack3)
    cells_land = (land0, land1, land2, land3)

    def ahead(place, d, size):
        return lax.rem(place + d, size)

    barrier = pltpu.get_barrier_semaphore()
    peers = [{"gx": ahead(place_x, d, lanes_x)} for d in range(1, lanes_x)]
    peers += [{"gy": ahead(place_y, d, lanes_y)} for d in range(1, lanes_y)]
    peers += [{"gz": ahead(place_z, d, lanes_z)} for d in (1, lanes_z - 1)]
    for peer in peers:
        pl.semaphore_signal(barrier, inc=1, device_id=peer, device_id_type=MESH)

    code = owner_ref[place_x, place_y, place_z]
    start_x, _, start_z = corner_of(start_ref, code, lanes_y, place_z)
    shift_z = place_z * BZ - start_z
    pick_x(lanes_x, place_x, start_x, logits_ref, cells_ref)

    order = (CLASSES,) + tuple(range(CLASSES))
    far_x = sorted(range(1, lanes_x), key=lambda d: -min(d, lanes_x - d))
    far_y = sorted(range(1, lanes_y), key=lambda d: -min(d, lanes_y - d))
    cell_copies = {
        (c, d): pltpu.make_async_remote_copy(
            src_ref=packed[c].at[d],
            dst_ref=cells_land[c].at[d],
            send_sem=cells_out.at[c, d],
            recv_sem=cells_in.at[c, d],
            device_id={"gx": ahead(place_x, d, lanes_x)},
            device_id_type=MESH,
        )
        for c in order
        for d in far_x
    }
    part_copies = {
        (c, d): pltpu.make_async_remote_copy(
            src_ref=parts.at[c, d],
            dst_ref=parts_land.at[c, d],
            send_sem=parts_out.at[c, d],
            recv_sem=parts_in.at[c, d],
            device_id={"gy": ahead(place_y, d, lanes_y)},
            device_id_type=MESH,
        )
        for c in order
        for d in far_y
    }
    rim_copies = [
        pltpu.make_async_remote_copy(
            src_ref=rims,
            dst_ref=rims_land.at[side],
            send_sem=rims_out.at[side],
            recv_sem=rims_in.at[side],
            device_id={"gz": ahead(place_z, d, lanes_z)},
            device_id_type=MESH,
        )
        for side, d in ((0, 1), (1, lanes_z - 1))
    ]
    for c in order:
        if c == CLASSES:
            pack_rims(lanes_x, shift_z, cells_ref, sums_ref, packed[c])
            pl.semaphore_wait(barrier, len(peers))
        else:
            pack_class(lanes_x, shift_z, c, cells_ref, packed[c])
        for d in far_x:
            cell_copies[c, d].start()

    sub = lax.broadcasted_iota(jnp.int32, (BX, BZ), 0)
    lane = lax.broadcasted_iota(jnp.int32, (BX, BZ), 1)
    cell_x = place_x * BX + sub
    cells_y = lanes_y * BY
    starts_y = []
    for p in range(lanes_x):
        source = lax.rem(place_x - p + lanes_x, lanes_x)
        code = owner_ref[source, place_y, place_z]
        start_x, start_y, start_z = corner_of(start_ref, code, lanes_y, place_z)
        starts_y.append(start_y)
        shift_z = place_z * BZ - start_z
        rim_z = lane % RIM + jnp.where(lane < BZ // 2, -RIM, BZ) + shift_z
        along_x = profile(cell_x - start_x, PX)
        plane_ref[p, 0] = along_x * profile(lane + shift_z, PZ)
        plane_ref[p, 1] = along_x * profile(rim_z, PZ, lane % (BZ // 2) < RIM * CLASSES)
        row = lax.broadcasted_iota(jnp.int32, (cells_y, BZ), 0)
        along_y_ref[p] = profile(row - start_y, PY)

    weight_ref[...] = jnp.zeros(weight_ref.shape, jnp.float32)
    cell_y = place_y * BY + lax.broadcasted_iota(jnp.int32, (BY, BZ), 0)

    def weigh(code, carry):
        for step in (-1, 0, 1):
            layer = jnp.clip(place_z + step, 0, lanes_z - 1)
            start_x, start_y, start_z = corner_of(start_ref, code, lanes_y, layer)
            along = profile(cell_y - start_y, PY)
            plane = profile(cell_x - start_x, PX) * profile(
                place_z * BZ + lane - start_z, PZ, layer == place_z + step
            )
            for y in range(BY):
                weight_ref[y] = weight_ref[y] + plane * along[y : y + 1]
        return carry

    lax.fori_loop(0, lanes_x * lanes_y, weigh, 0)

    def blend(c):
        kind = 0 if c < CLASSES else 1
        for d in far_y + [0]:
            base = ahead(place_y, d, lanes_y) * BY

            def step(y, carry):
                row = base + y
                total = None
                for p in range(lanes_x):
                    q = jnp.clip(row - starts_y[p], 0, PY - 1)
                    held = packed[c] if p == 0 else cells_land[c]
                    if c < CLASSES:
                        cells = held[p, q].astype(jnp.float32)
                    else:
                        half = jnp.where(q >= FOLD, 1, 0)
                        cells = held[p, q - half * FOLD].astype(jnp.float32)
                        swapped = pltpu.roll(cells, BZ // 2, 1)
                        cells = jnp.where(lane // (BZ // 2) == half, cells, swapped)
                    term = cells * (plane_ref[p, kind] * along_y_ref[p, pl.ds(row, 1)])
                    total = term if total is None else total + term
                parts[c, d, y] = total
                return carry

            lax.fori_loop(0, BY, step, 0, unroll=2)
            if d:
                part_copies[c, d].start()

    def gathered(c, y):
        total = parts[c, 0, y]
        for d in range(1, lanes_y):
            total = total + parts_land[c, d, y]
        return total

    for c in order:
        for d in far_x:
            cell_copies[c, d].wait_recv()
        blend(c)
        if c == 0:
            for d in far_y:
                part_copies[CLASSES, d].wait_recv()

            def add_rims(y, carry):
                rims[y] = gathered(CLASSES, y)
                return carry

            lax.fori_loop(0, BY, add_rims, 0)
            for copy in rim_copies:
                copy.start()

    for copy in rim_copies:
        copy.wait_recv()
    for c in range(CLASSES):
        for d in far_y:
            part_copies[c, d].wait_recv()

    low_lanes = (lane < RIM) & (place_z > 0)
    high_lanes = (lane >= BZ - RIM) & (place_z < lanes_z - 1)

    def finish(y, carry):
        scale = 1.0 / weight_ref[y]
        below = rims_land[0, y]
        above = rims_land[1, y]
        scores = []
        for c in range(CLASSES):
            low = pltpu.roll(below, BZ // 2 - RIM * c, 1)
            high = pltpu.roll(above, BZ - RIM - RIM * c, 1)
            total = gathered(c, y) + jnp.where(low_lanes, low, 0.0)
            total = total + jnp.where(high_lanes, high, 0.0)
            scores.append(total * scale)
        top = functools.reduce(jnp.maximum, scores)
        powers = [jnp.exp(s - top) for s in scores]
        norm = 1.0 / functools.reduce(jnp.add, powers)
        for c in range(CLASSES):
            out_ref[y, c] = powers[c] * norm
        return carry

    lax.fori_loop(0, BY, finish, 0, unroll=4)
    for copy in list(cell_copies.values()) + list(part_copies.values()) + rim_copies:
        copy.wait_send()


VMEM = pl.BlockSpec(memory_space=pltpu.VMEM)
SMEM = pl.BlockSpec(memory_space=pltpu.SMEM)


def per_device(patch_logits, patch_start, patch_owner):
    lanes_x = lax.axis_size("gx")
    lanes_y = lax.axis_size("gy")
    lanes_z = lax.axis_size("gz")
    row_shapes = [(lanes_x, PY, BX, BZ)] * CLASSES + [(lanes_x, FOLD, BX, BZ)]
    parts_shape = (ROWS, lanes_y, BY, BX, BZ)
    probs = pl.pallas_call(
        functools.partial(blend_kernel, lanes_x, lanes_y, lanes_z),
        out_shape=jax.ShapeDtypeStruct((BY, CLASSES, BX, BZ), jnp.float32),
        in_specs=[SMEM, SMEM, VMEM],
        out_specs=VMEM,
        scratch_shapes=[
            pltpu.VMEM((lanes_x, lanes_y * BY, BZ), jnp.float32),
            pltpu.VMEM((lanes_x, 2, BX, BZ), jnp.float32),
            pltpu.VMEM((BY, BX, BZ), jnp.float32),
            pltpu.VMEM((lanes_x * BX, PY * CLASSES * PZ), jnp.bfloat16),
            pltpu.VMEM((FOLD, lanes_x * BX, BZ), jnp.float32),
            *[pltpu.VMEM(shape, jnp.bfloat16) for shape in row_shapes * 2],
            pltpu.VMEM(parts_shape, jnp.float32),
            pltpu.VMEM(parts_shape, jnp.float32),
            pltpu.VMEM((BY, BX, BZ), jnp.float32),
            pltpu.VMEM((2, BY, BX, BZ), jnp.float32),
            pltpu.SemaphoreType.DMA((ROWS, lanes_x)),
            pltpu.SemaphoreType.DMA((ROWS, lanes_x)),
            pltpu.SemaphoreType.DMA((ROWS, lanes_y)),
            pltpu.SemaphoreType.DMA((ROWS, lanes_y)),
            pltpu.SemaphoreType.DMA((2,)),
            pltpu.SemaphoreType.DMA((2,)),
        ],
        compiler_params=pltpu.CompilerParams(collective_id=0, has_side_effects=True),
    )(patch_start, patch_owner, patch_logits[0, 0, 0])
    return jnp.transpose(probs, (2, 0, 1, 3))


def solution(mesh):
    return jax.shard_map(
        per_device,
        mesh=mesh,
        in_specs=(P("gx", "gy", "gz", None, None), P(), P()),
        out_specs=P("gx", "gy", None, "gz"),
        check_vma=False,
    )
```

```python
import functools

import jax
import jax.numpy as jnp
from jax import lax
from jax.experimental import pallas as pl
from jax.experimental.pallas import tpu as pltpu
from jax.sharding import PartitionSpec as P

CLASSES = 3
BX = 8
BY = 32
BZ = 128
HALO = 8
PX = 24
PY = 48
PZ = 144
RIM = PZ - BZ
ROWS = CLASSES + 1
GROUP = 8
FOLD = PY // 2
MESH = pl.DeviceIdType.MESH


def profile(offsets, length, keep=True):
    inside = (offsets >= 0) & (offsets < length) & keep
    centre = (length - 1) / 2.0
    spread = length / 4.0
    values = jnp.exp((offsets.astype(jnp.float32) - centre) ** 2 * (-0.5 / (spread * spread)))
    return jnp.where(inside, values, 0.0)


def corner_of(start_ref, code, lanes_y, layer):
    return [start_ref[code // lanes_y, k, layer, code % lanes_y] for k in range(3)]


def pick_x(lanes_x, place_x, start_x, logits_ref, cells_ref):
    rows = lanes_x * BX
    r = lax.broadcasted_iota(jnp.int32, (rows, PX), 0)
    p = lax.broadcasted_iota(jnp.int32, (rows, PX), 1)
    x = r + place_x * BX
    x = jnp.where(x >= rows, x - rows, x)
    pick = jnp.where(x - start_x == p, 1.0, 0.0).astype(jnp.bfloat16)
    width = GROUP * CLASSES * PZ
    for g in range(PY // GROUP):
        lanes = slice(g * width, (g + 1) * width)
        cells = jnp.dot(pick, logits_ref[:, lanes], preferred_element_type=jnp.float32)
        cells_ref[:, lanes] = cells.astype(jnp.bfloat16)


def lines_of(cells_ref, lines, source, phase):
    k = lax.broadcasted_iota(jnp.int32, (2 * BZ, BZ), 0)
    move = jnp.where(k - phase * RIM == source, 1.0, 0.0).astype(jnp.bfloat16)
    starts = [line * PZ - phase * RIM for line in lines]
    cells = jnp.concatenate([cells_ref[:, at : at + 2 * BZ] for at in starts], axis=0)
    return jnp.dot(cells, move, preferred_element_type=jnp.float32)


def pack_rims(lanes_x, shift_z, cells_ref, sums_ref, out_ref):
    rows = lanes_x * BX
    phases = BZ // RIM
    n = lax.broadcasted_iota(jnp.int32, (2 * BZ, BZ), 1)
    source = n + shift_z + jnp.where(n + shift_z < RIM, BZ, -RIM)
    source = jnp.where(n < RIM, source, -4 * BZ)
    sums_ref[...] = jnp.zeros(sums_ref.shape, jnp.float32)
    for phase in range(phases):
        lines = [i for i in range(PY * CLASSES) if i % phases == phase]
        moved = lines_of(cells_ref, lines, source, phase)
        for i, line in enumerate(lines):
            y, c = divmod(line, CLASSES)
            rim = moved[i * rows : (i + 1) * rows]
            at = RIM * c + BZ // 2 * (y // FOLD)
            rim = pltpu.roll(rim, at, 1) if at else rim
            sums_ref[y % FOLD] = sums_ref[y % FOLD] + rim

    def convert(y, carry):
        sums = sums_ref[y].astype(jnp.bfloat16)
        for t in range(lanes_x):
            out_ref[t, y] = sums[t * BX : (t + 1) * BX]
        return carry

    lax.fori_loop(0, FOLD, convert, 0, unroll=2)


def pack_class(lanes_x, shift_z, c, cells_ref, out_ref):
    rows = lanes_x * BX
    phases = BZ // RIM
    source = lax.broadcasted_iota(jnp.int32, (2 * BZ, BZ), 1) + shift_z
    for phase in range(phases):
        ys = [y for y in range(PY) if (y * CLASSES + c) % phases == phase]
        moved = lines_of(cells_ref, [y * CLASSES + c for y in ys], source, phase)
        moved = moved.astype(jnp.bfloat16)
        for i, y in enumerate(ys):
            for t in range(lanes_x):
                at = i * rows + t * BX
                out_ref[t, y] = moved[at : at + BX]


def blend_kernel(
    lanes_x, lanes_y, lanes_z,
    start_ref, owner_ref, logits_ref, out_ref, along_y_ref, plane_ref, weight_ref,
    cells_ref, sums_ref, pack0, pack1, pack2, pack3, land0, land1, land2, land3, parts, parts_land, rims, rims_land,
    cells_out, cells_in, parts_out, parts_in, rims_out, rims_in,
):
    place_x = lax.axis_index("gx")
    place_y = lax.axis_index("gy")
    place_z = lax.axis_index("gz")

    packed = (pack0, pack1, pack2, pack3)
    cells_land = (land0, land1, land2, land3)

    def ahead(place, d, size):
        return lax.rem(place + d, size)

    barrier = pltpu.get_barrier_semaphore()
    peers = [{"gx": ahead(place_x, d, lanes_x)} for d in range(1, lanes_x)]
    peers += [{"gy": ahead(place_y, d, lanes_y)} for d in range(1, lanes_y)]
    peers += [{"gz": ahead(place_z, d, lanes_z)} for d in (1, lanes_z - 1)]
    for peer in peers:
        pl.semaphore_signal(barrier, inc=1, device_id=peer, device_id_type=MESH)

    code = owner_ref[place_x, place_z, place_y]
    start_x, _, start_z = corner_of(start_ref, code, lanes_y, place_z)
    shift_z = place_z * BZ - start_z
    pick_x(lanes_x, place_x, start_x, logits_ref, cells_ref)

    order = (0, CLASSES) + tuple(range(1, CLASSES))
    far_x = sorted(range(1, lanes_x), key=lambda d: -min(d, lanes_x - d))
    far_y = sorted(range(1, lanes_y), key=lambda d: -min(d, lanes_y - d))
    cell_copies = {
        (c, d): pltpu.make_async_remote_copy(
            src_ref=packed[c].at[d],
            dst_ref=cells_land[c].at[d],
            send_sem=cells_out.at[c, d],
            recv_sem=cells_in.at[c, d],
            device_id={"gx": ahead(place_x, d, lanes_x)},
            device_id_type=MESH,
        )
        for c in order
        for d in far_x
    }
    part_copies = {
        (c, d): pltpu.make_async_remote_copy(
            src_ref=parts.at[c, d],
            dst_ref=parts_land.at[c, d],
            send_sem=parts_out.at[c, d],
            recv_sem=parts_in.at[c, d],
            device_id={"gy": ahead(place_y, d, lanes_y)},
            device_id_type=MESH,
        )
        for c in order
        for d in far_y
    }
    rim_copies = [
        pltpu.make_async_remote_copy(
            src_ref=rims,
            dst_ref=rims_land.at[side],
            send_sem=rims_out.at[side],
            recv_sem=rims_in.at[side],
            device_id={"gz": ahead(place_z, d, lanes_z)},
            device_id_type=MESH,
        )
        for side, d in ((0, 1), (1, lanes_z - 1))
    ]
    for c in order:
        if c == CLASSES:
            pack_rims(lanes_x, shift_z, cells_ref, sums_ref, packed[c])
        else:
            pack_class(lanes_x, shift_z, c, cells_ref, packed[c])
        if c == order[0]:
            pl.semaphore_wait(barrier, len(peers))
        for d in far_x:
            cell_copies[c, d].start()

    sub = lax.broadcasted_iota(jnp.int32, (BX, BZ), 0)
    lane = lax.broadcasted_iota(jnp.int32, (BX, BZ), 1)
    cell_x = place_x * BX + sub
    cells_y = lanes_y * BY
    starts_y = []
    for p in range(lanes_x):
        source = lax.rem(place_x - p + lanes_x, lanes_x)
        code = owner_ref[source, place_z, place_y]
        start_x, start_y, start_z = corner_of(start_ref, code, lanes_y, place_z)
        starts_y.append(start_y)
        shift_z = place_z * BZ - start_z
        rim_z = lane % RIM + jnp.where(lane < BZ // 2, -RIM, BZ) + shift_z
        along_x = profile(cell_x - start_x, PX)
        plane_ref[p, 0] = along_x * profile(lane + shift_z, PZ)
        plane_ref[p, 1] = along_x * profile(rim_z, PZ, lane % (BZ // 2) < RIM * CLASSES)
        row = lax.broadcasted_iota(jnp.int32, (cells_y, BZ), 0)
        along_y_ref[p] = profile(row - start_y, PY)

    weight_ref[...] = jnp.zeros(weight_ref.shape, jnp.float32)
    cell_y = place_y * BY + lax.broadcasted_iota(jnp.int32, (BY, BZ), 0)

    def weigh(code, carry):
        for step in (-1, 0, 1):
            layer = jnp.clip(place_z + step, 0, lanes_z - 1)
            start_x, start_y, start_z = corner_of(start_ref, code, lanes_y, layer)
            along = profile(cell_y - start_y, PY)
            plane = profile(cell_x - start_x, PX) * profile(
                place_z * BZ + lane - start_z, PZ, layer == place_z + step
            )
            for y in range(BY):
                weight_ref[y] = weight_ref[y] + plane * along[y : y + 1]
        return carry

    lax.fori_loop(0, lanes_x * lanes_y, weigh, 0)

    def blend(c):
        kind = 0 if c < CLASSES else 1
        for d in far_y + [0]:
            base = ahead(place_y, d, lanes_y) * BY

            def step(y, carry):
                row = base + y
                total = None
                for p in range(lanes_x):
                    q = jnp.clip(row - starts_y[p], 0, PY - 1)
                    held = packed[c] if p == 0 else cells_land[c]
                    if c < CLASSES:
                        cells = held[p, q].astype(jnp.float32)
                    else:
                        half = jnp.where(q >= FOLD, 1, 0)
                        cells = held[p, q - half * FOLD].astype(jnp.float32)
                        swapped = pltpu.roll(cells, BZ // 2, 1)
                        cells = jnp.where(lane // (BZ // 2) == half, cells, swapped)
                    term = cells * (plane_ref[p, kind] * along_y_ref[p, pl.ds(row, 1)])
                    total = term if total is None else total + term
                parts[c, d, y] = total
                return carry

            lax.fori_loop(0, BY, step, 0, unroll=2)
            if d:
                part_copies[c, d].start()

    def gathered(c, y):
        total = parts[c, 0, y]
        for d in range(1, lanes_y):
            total = total + parts_land[c, d, y]
        return total

    low_lanes = (lane < RIM) & (place_z > 0)
    high_lanes = (lane >= BZ - RIM) & (place_z < lanes_z - 1)

    def add_rims(y, carry):
        rims[y] = gathered(CLASSES, y)
        return carry

    def rim_of(c, y):
        low = pltpu.roll(rims_land[0, y], BZ // 2 - RIM * c, 1)
        high = pltpu.roll(rims_land[1, y], BZ - RIM - RIM * c, 1)
        return jnp.where(low_lanes, low, jnp.where(high_lanes, high, 0.0))

    def early(y, carry):
        weight_ref[y] = 1.0 / weight_ref[y]
        for c in range(CLASSES - 1):
            parts[c, 0, y] = (gathered(c, y) + rim_of(c, y)) * weight_ref[y]
        parts[CLASSES - 1, 0, y] = parts[CLASSES - 1, 0, y] + rim_of(CLASSES - 1, y)
        return carry

    def finish(y, carry):
        scores = [parts[c, 0, y] for c in range(CLASSES - 1)]
        scores.append(gathered(CLASSES - 1, y) * weight_ref[y])
        top = functools.reduce(jnp.maximum, scores)
        powers = [jnp.exp(s - top) for s in scores]
        norm = 1.0 / functools.reduce(jnp.add, powers)
        for c in range(CLASSES):
            out_ref[y, c] = powers[c] * norm
        return carry

    for c in order:
        for d in far_x:
            cell_copies[c, d].wait_recv()
        blend(c)
        if c == 1:
            for d in far_y:
                part_copies[CLASSES, d].wait_recv()
            lax.fori_loop(0, BY, add_rims, 0, unroll=4)
            for copy in rim_copies:
                copy.start()

    for copy in rim_copies:
        copy.wait_recv()
    for c in range(CLASSES - 1):
        for d in far_y:
            part_copies[c, d].wait_recv()
    lax.fori_loop(0, BY, early, 0, unroll=4)
    for d in far_y:
        part_copies[CLASSES - 1, d].wait_recv()
    lax.fori_loop(0, BY, finish, 0, unroll=8)
    for copy in list(cell_copies.values()) + list(part_copies.values()) + rim_copies:
        copy.wait_send()


VMEM = pl.BlockSpec(memory_space=pltpu.VMEM)
SMEM = pl.BlockSpec(memory_space=pltpu.SMEM)


def per_device(patch_logits, patch_start, patch_owner):
    lanes_x = lax.axis_size("gx")
    lanes_y = lax.axis_size("gy")
    lanes_z = lax.axis_size("gz")
    row_shapes = [(lanes_x, PY, BX, BZ)] * CLASSES + [(lanes_x, FOLD, BX, BZ)]
    parts_shape = (ROWS, lanes_y, BY, BX, BZ)
    probs = pl.pallas_call(
        functools.partial(blend_kernel, lanes_x, lanes_y, lanes_z),
        out_shape=jax.ShapeDtypeStruct((BY, CLASSES, BX, BZ), jnp.float32),
        in_specs=[SMEM, SMEM, VMEM],
        out_specs=VMEM,
        scratch_shapes=[
            pltpu.VMEM((lanes_x, lanes_y * BY, BZ), jnp.float32),
            pltpu.VMEM((lanes_x, 2, BX, BZ), jnp.float32),
            pltpu.VMEM((BY, BX, BZ), jnp.float32),
            pltpu.VMEM((lanes_x * BX, PY * CLASSES * PZ), jnp.bfloat16),
            pltpu.VMEM((FOLD, lanes_x * BX, BZ), jnp.float32),
            *[pltpu.VMEM(shape, jnp.bfloat16) for shape in row_shapes * 2],
            pltpu.VMEM(parts_shape, jnp.float32),
            pltpu.VMEM(parts_shape, jnp.float32),
            pltpu.VMEM((BY, BX, BZ), jnp.float32),
            pltpu.VMEM((2, BY, BX, BZ), jnp.float32),
            pltpu.SemaphoreType.DMA((ROWS, lanes_x)),
            pltpu.SemaphoreType.DMA((ROWS, lanes_x)),
            pltpu.SemaphoreType.DMA((ROWS, lanes_y)),
            pltpu.SemaphoreType.DMA((ROWS, lanes_y)),
            pltpu.SemaphoreType.DMA((2,)),
            pltpu.SemaphoreType.DMA((2,)),
        ],
        compiler_params=pltpu.CompilerParams(collective_id=0, has_side_effects=True),
    )(
        jnp.transpose(patch_start, (0, 3, 2, 1)),
        jnp.transpose(patch_owner, (0, 2, 1)),
        patch_logits[0, 0, 0],
    )
    return jnp.transpose(probs, (2, 0, 1, 3))


def solution(mesh):
    return jax.shard_map(
        per_device,
        mesh=mesh,
        in_specs=(P("gx", "gy", "gz", None, None), P(), P()),
        out_specs=P("gx", "gy", None, "gz"),
        check_vma=False,
    )
```
